32 devices in a mesh: grid: 8 (over z, y), atom: 4 (over x, core).
Axes of the slice: x: 2, y: 2, z: 4, core: 2. Of those that a mesh axis runs over, the one named last changes fastest.
Arguments:
- weights: float32 [524288], P(('grid', 'atom')), may hold values from 0.25 to 4
- target: float32 [524288], P(('grid', 'atom')), may hold values from -6 to 6
- coupling: float32 [524288], P(('grid', 'atom')), may hold values from -0.9 to 0.9
- multipole_basis: float32 [25, 524288], P(None, ('grid', 'atom')), may hold values from -6 to 6
- rho_hist: float32 [8, 524288], P(None, ('grid', 'atom')), may hold values from -6 to 6
- res_hist: float32 [8, 524288], P(None, ('grid', 'atom')), may hold values from -6 to 6
- batch_atom: int32 [2048], P(('grid', 'atom')), may hold values from 0 to 2047
- owner_slot: int32 [2048], replicated, may hold values from 0 to 2047, each once
- slot_index: int32 [2], replicated, may hold values from 0 to 7
Outputs:
- density: float32 [524288], P(('grid', 'atom'))
- moments: float32 [25, 2048], P(None, 'atom')
The draws below stay inside these ranges and needn't reach their ends.
Inputs may be any that keep to these rules, and one draw needn't show every extreme that they name: `owner_slot`: each slot 0 to 2047 belongs to exactly one atom.
All inputs are finite; a program needn't handle non-finite values.
Results may differ from the reference program's by a relative error of at most 0.00011.
Values sent between devices are 32-bit elements; how exact they have to be, the bound alone decides.
A program may use at most 64 MiB of HBM per device.

```python
import math
import jax
import jax.numpy as jnp
import numpy as np
from jax import lax

H = 8
LM = 25
BATCH = 256
ITERS = 2
POINTS = 524288
BATCHES = 2048
ATOMS = 2048
ATOM_PTS = 256


def place_ends(result, key, least, largest):
    spot = [jax.random.randint(jax.random.fold_in(key, axis), (), 0, length) for axis, length in enumerate(result.shape)]
    longest = result.shape.index(max(result.shape))
    neighbour = spot[:longest] + [(spot[longest] + 1) % result.shape[longest]] + spot[longest + 1:]
    return result.at[tuple(spot)].set(least).at[tuple(neighbour)].set(largest)


def levels(own_key, dims, pieces, smallest, top_value):
    def one(position, shards_of):
        heights = jax.random.uniform(jax.random.fold_in(jax.random.fold_in(own_key, 6), position), (shards_of,), jnp.float32, smallest / len(pieces), top_value / len(pieces))
        return jnp.repeat(jnp.exp(heights), dims[position] // shards_of).reshape((-1,) + (1,) * (len(dims) - position - 1))

    gain = one(*pieces[0])
    for cut in pieces[1:]:
        gain = gain * one(*cut)
    return gain


def noise(stream_key, shape, scale, reach, shards=(), held_as=jnp.bfloat16):
    gain = levels(stream_key, shape, shards, -0.22, 0.18) if shards else 1.0
    entries = jax.random.normal(stream_key, shape, jnp.float32) * scale * gain
    return jnp.minimum(jnp.maximum(entries, -reach), reach).astype(held_as)


def setup_inputs(seed: int = 0) -> dict:
    splits = jax.random.split(jax.random.key(seed), 10)
    return {
        "weights": jnp.clip(jnp.exp(math.log(4.0) - 2.7725887 * jax.random.uniform(splits[0], (POINTS,), jnp.float32) ** levels(splits[0], (POINTS,), ((0, 32),), -0.2, 0.2)), 0.25, 4.0),
        "target": noise(splits[1], (POINTS,), 1.0, 6.0, ((0, 32),), jnp.float32),
        "coupling": jnp.clip(jax.random.uniform(splits[2], (POINTS,), jnp.float32, -0.9, 0.9) * levels(splits[2], (POINTS,), ((0, 32),), -0.4, 0.0), -0.9, 0.9),
        "multipole_basis": noise(splits[3], (LM, POINTS), 1.0, 6.0, ((1, 32),), jnp.float32),
        "rho_hist": noise(splits[4], (H, POINTS), 1.0, 6.0, ((1, 32),), jnp.float32),
        "res_hist": noise(splits[5], (H, POINTS), 1.0, 6.0, ((1, 32),), jnp.float32),
        "batch_atom": place_ends(jax.random.randint(splits[6], (BATCHES,), 0, ATOMS), jax.random.fold_in(splits[6], 1), 0, ATOMS - 1).astype(jnp.int32),
        "owner_slot": jax.random.permutation(splits[7], ATOMS).astype(jnp.int32),
        "slot_index": jax.random.randint(splits[8], (ITERS,), 0, H).astype(jnp.int32),
    }


damping_table = np.array([1.0 / (1 + degree) for degree in range(5) for order in range(2 * degree + 1)], dtype=np.float32)
mixing_beta = 0.5
ridge_share = 0.1

def mixing_weights(intersect):
    hist_len = intersect.shape[0]
    ridge_val = ridge_share * jnp.trace(intersect) / hist_len
    shifted = intersect + ridge_val * jnp.eye(hist_len, dtype=intersect.dtype)
    factor = jnp.linalg.cholesky(shifted)
    forward = []
    for row_at in range(hist_len):
        entry_val = 1.0
        for col_at in range(row_at):
            entry_val = entry_val - factor[row_at, col_at] * forward[col_at]
        forward.append(entry_val / factor[row_at, row_at])
    backward = [None] * hist_len
    for row_at in reversed(range(hist_len)):
        entry_val = forward[row_at]
        for col_at in range(row_at + 1, hist_len):
            entry_val = entry_val - factor[col_at, row_at] * backward[col_at]
        backward[row_at] = entry_val / factor[row_at, row_at]
    solved = jnp.stack(backward)
    return solved / jnp.sum(solved)

def reference(weights, target, coupling, multipole_basis, rho_hist, res_hist, batch_atom, owner_slot, slot_index):
    hi_prec = lax.Precision.HIGHEST
    damping = jnp.asarray(damping_table, dtype=weights.dtype)
    batch_slot = owner_slot[batch_atom].astype(jnp.int32)
    basis_blocks = multipole_basis.reshape(LM, BATCHES, BATCH)
    density = None
    moments = None
    for iteration in range(ITERS):
        intersect = jnp.dot(res_hist * weights[None, :], res_hist.T, precision=hi_prec)
        coeffs = mixing_weights(intersect)
        rho_mix = jnp.dot(coeffs, rho_hist, precision=hi_prec)
        res_mix = jnp.dot(coeffs, res_hist, precision=hi_prec)
        per_batch = lax.optimization_barrier(jnp.sum((weights * res_mix).reshape(1, BATCHES, BATCH) * basis_blocks, axis=2))
        moments = jax.ops.segment_sum(per_batch.T, batch_slot, num_segments=ATOMS).T / jnp.sqrt(jnp.float32(ATOM_PTS)).astype(weights.dtype)
        at_batch = damping[:, None] * moments[:, batch_slot]
        correct = lax.optimization_barrier(jnp.sum(at_batch[:, :, None] * basis_blocks, axis=0)).reshape(POINTS)
        density = rho_mix + mixing_beta * (res_mix - correct)
        res_new = target + coupling * jnp.tanh(density) - density
        where = slot_index[iteration]
        rho_hist = rho_hist.at[where].set(density)
        res_hist = res_hist.at[where].set(res_new)
    return (density, moments)
```

```python
import functools
import math

import jax
import jax.numpy as jnp
from jax import lax
from jax.experimental import pallas as pl
from jax.experimental.pallas import tpu as pltpu
from jax.sharding import PartitionSpec as P

MESH = pl.DeviceIdType.MESH
LANES = 128
SUBS = 8
mixing_beta = 0.5
ridge_share = 0.1
F32 = jnp.float32


def solve_coeffs(entry, hist_len):
    trace = entry[0][0]
    for i in range(1, hist_len):
        trace = trace + entry[i][i]
    ridge = (ridge_share / hist_len) * trace
    low = [[entry[i][j] for j in range(i + 1)] for i in range(hist_len)]
    for i in range(hist_len):
        low[i][i] = low[i][i] + ridge
    inverse = [None] * hist_len
    factor = [[None] * hist_len for _ in range(hist_len)]
    forward = [jnp.ones_like(trace) for _ in range(hist_len)]
    for j in range(hist_len):
        inverse[j] = 1.0 / low[j][j]
        for i in range(j + 1, hist_len):
            factor[i][j] = low[i][j] * inverse[j]
        for i in range(j + 1, hist_len):
            forward[i] = forward[i] - factor[i][j] * forward[j]
            for k in range(j + 1, i + 1):
                low[i][k] = low[i][k] - factor[i][j] * low[k][j]
    backward = [forward[i] * inverse[i] for i in range(hist_len)]
    for j in reversed(range(hist_len)):
        for i in range(j):
            backward[i] = backward[i] - factor[j][i] * backward[j]
    total = backward[0]
    for i in range(1, hist_len):
        total = total + backward[i]
    return [backward[i] / total for i in range(hist_len)]


def kernel(
    cfg,
    batch_atom,
    owner_slot,
    slot_index,
    w_hbm,
    target_hbm,
    coupling_hbm,
    basis_hbm,
    rho_hbm,
    res_hbm,
    density_out,
    moments_out,
    w,
    target,
    coupling,
    basis,
    rho,
    res,
    fresh,
    fresh_w,
    row_bufs,
    moment_bufs,
    masks,
    mixed,
    load_sem,
    send_sem,
    recv_sem,
):
    iters, hist_len, harmonics, batches, width, owned, groups, members, scale = cfg
    devices = groups * members
    tiles = w.shape[0]
    per_batch = width // LANES
    half = LANES // 2
    pairs = devices // 2
    my_group = lax.axis_index("grid")
    my_member = lax.axis_index("atom")
    me = my_group * members + my_member

    def peer(step):
        spot = lax.rem(me + step, devices)
        return spot, (lax.div(spot, members), lax.rem(spot, members))

    barrier = pltpu.get_barrier_semaphore()

    @pl.loop(1, devices)
    def _(step):
        pl.semaphore_signal(barrier, inc=1, device_id=peer(step)[1], device_id_type=MESH)

    loads = [
        pltpu.make_async_copy(src, dst, load_sem.at[k])
        for k, (src, dst) in enumerate(
            ((res_hbm, res), (w_hbm, w), (basis_hbm, basis), (rho_hbm, rho), (target_hbm, target), (coupling_hbm, coupling))
        )
    ]
    for load in loads:
        load.start()

    lane = lax.broadcasted_iota(jnp.int32, (SUBS, LANES), 1)
    sub = lax.broadcasted_iota(jnp.int32, (SUBS, LANES), 0)
    lane_row = lax.broadcasted_iota(jnp.int32, (1, LANES), 1)

    slot_row = jnp.zeros((1, LANES), F32)
    slot_cols = []
    for block in range(batches // SUBS):
        col = jnp.zeros((SUBS, LANES), F32)
        for at in range(SUBS):
            b = block * SUBS + at
            slot = owner_slot[batch_atom[b]].astype(F32)
            slot_row = jnp.where(lane_row == half + b, slot, slot_row)
            col = jnp.where(sub == at, slot, col)
        slot_cols.append(col)
    slot_col = jnp.concatenate(slot_cols, axis=0)

    def lane_tile(t):
        return pl.ds(pl.multiple_of(t * LANES, LANES), LANES)

    def exchange(buf, which):
        def copy(step, spot):
            dst, device = peer(step)
            return pltpu.make_async_remote_copy(
                src_ref=buf.at[me],
                dst_ref=buf.at[spot],
                send_sem=send_sem.at[which, step],
                recv_sem=recv_sem.at[which, spot],
                device_id=device,
                device_id_type=MESH,
            )

        @pl.loop(1, devices)
        def _(step):
            copy(step, me).start()

        def wait():
            @pl.loop(1, devices)
            def _(step):
                copy(step, lax.rem(me - step + devices, devices)).wait_recv()

            @pl.loop(1, devices)
            def _(step):
                copy(step, me).wait_send()

        return wait

    def total_row(buf):
        total = buf[0]
        for spot in range(1, devices):
            total = total + buf[spot]
        return total

    def splat(row, k):
        return jnp.broadcast_to(row[:, k : k + 1], (1, LANES))

    shifts = hist_len // 2 + 1
    entry = None
    for iteration in range(iters):
        row_buf = row_bufs.at[iteration]
        moment_buf = moment_bufs.at[iteration]
        last = iteration == iters - 1

        if iteration == 0:
            loads[0].wait()
            loads[1].wait()

            def gram(step, acc):
                acc = list(acc)
                for u in range(8):
                    t = step * 8 + u
                    x = res[:, lane_tile(t)]
                    y = x * w[pl.ds(t, 1), :]
                    for r in range(shifts):
                        acc[r] = acc[r] + y * (pltpu.roll(x, r, 0) if r else x)
                return tuple(acc)

            acc = lax.fori_loop(0, tiles // 8, gram, tuple(jnp.zeros((SUBS, LANES), F32) for _ in range(shifts)))
            packed = jnp.zeros((SUBS, LANES), F32)
            for r in range(shifts):
                packed = jnp.where(lane == hist_len * r + sub, jnp.sum(acc[r], axis=1, keepdims=True), packed)
            row_buf[pl.ds(me, 1)] = (jnp.sum(packed, axis=0, keepdims=True) + slot_row)[None]
            pl.semaphore_wait(barrier, devices - 1)
        else:
            if iteration == 1:
                pass
            slot = slot_index[iteration - 1]
            replaced = sub == slot

            def refresh(step, acc):
                for u in range(8):
                    t = step * 8 + u
                    new_res = jnp.where(replaced, fresh[pl.ds(t, 1), :], res[:, lane_tile(t)])
                    new_rho = jnp.where(replaced, density_out[pl.ds(t, 1), :], rho[:, lane_tile(t)])
                    res[:, lane_tile(t)] = new_res
                    rho[:, lane_tile(t)] = new_rho
                    acc = acc + fresh_w[pl.ds(t, 1), :] * new_res
                return acc

            acc = lax.fori_loop(0, tiles // 8, refresh, jnp.zeros((SUBS, LANES), F32))
            packed = jnp.where(lane == sub, jnp.sum(acc, axis=1, keepdims=True), 0.0)
            row_buf[pl.ds(me, 1)] = jnp.sum(packed, axis=0, keepdims=True)[None]
        exchange(row_buf, 2 * iteration)()

        row = total_row(row_buf)
        if iteration == 0:
            entry = [[None] * (i + 1) for i in range(hist_len)]
            for i in range(hist_len):
                for j in range(i + 1):
                    r = i - j
                    at = hist_len * r + i if r < shifts else hist_len * (hist_len - r) + j
                    entry[i][j] = splat(row, at)
        else:
            news = [splat(row, k) for k in range(hist_len)]
            slot_vec = jnp.zeros((1, LANES), jnp.int32) + slot
            entry = [
                [
                    jnp.where(slot_vec == i, news[j], jnp.where(slot_vec == j, news[i], entry[i][j]))
                    for j in range(i + 1)
                ]
                for i in range(hist_len)
            ]
        coeffs = solve_coeffs(entry, hist_len)
        coeff_col = jnp.zeros((SUBS, LANES), F32)
        for i in range(hist_len):
            coeff_col = jnp.where(sub == i, coeffs[i], coeff_col)

        if iteration == 0:
            loads[2].wait()

        def moment_step(step, acc):
            lo, hi = acc
            for u in range(4):
                b = step * 4 + u
                parts = [None] * 4
                for v in range(per_batch):
                    t = b * per_batch + v
                    x = jnp.sum(coeff_col * res[:, lane_tile(t)], axis=0, keepdims=True) * w[pl.ds(t, 1), :]
                    for g in range(4):
                        rows = basis[g * SUBS : (g + 1) * SUBS, lane_tile(t)] if g < 3 else basis[24:25, lane_tile(t)]
                        term = rows * x
                        parts[g] = term if v == 0 else parts[g] + term
                sums = [jnp.sum(part, axis=1, keepdims=True) for part in parts]
                lo = jnp.where(lane == b, sums[0], jnp.where(lane == b + half, sums[2], lo))
                hi = jnp.where(lane == b, sums[1], jnp.where(lane == b + half, sums[3], hi))
            return lo, hi

        zero = jnp.zeros((SUBS, LANES), F32)
        lo, hi = lax.fori_loop(0, batches // 4, moment_step, (zero, zero))
        moment_buf[pl.ds(me, 1)] = jnp.concatenate([lo, hi], axis=0)[None]
        wait = exchange(moment_buf, 2 * iteration + 1)

        if iteration == 0:
            base = (my_member * owned).astype(F32)
            wide = lax.broadcasted_iota(jnp.int32, (owned, LANES), 0).astype(F32) + base

            @pl.loop(0, pairs)
            def _(q):
                even = row_buf[2 * q]
                odd = row_buf[2 * q + 1]
                slots = jnp.where(lane_row < half, pltpu.roll(even, half, 1), odd)
                masks[0:batches, lane_tile(q)] = jnp.where(slot_col == slots, 1.0, 0.0).astype(jnp.bfloat16)
                masks[batches : batches + owned, lane_tile(q)] = jnp.where(wide == slots, 1.0, 0.0).astype(jnp.bfloat16)

            for load in loads[3:]:
                load.wait()
        wait()

        lane16 = lax.broadcasted_iota(jnp.int32, (2 * SUBS, LANES), 1)

        @pl.loop(0, pairs)
        def _(q):
            even = moment_buf[2 * q]
            odd = moment_buf[2 * q + 1]
            first = jnp.where(lane16 < half, even, pltpu.roll(odd, half, 1))
            second = jnp.where(lane16 < half, pltpu.roll(even, half, 1), odd)
            rest = jnp.concatenate([first, second], axis=0)
            for part in range(3):
                piece = rest.astype(jnp.bfloat16)
                mixed[part * 32 : (part + 1) * 32, lane_tile(q)] = piece
                rest = rest - piece.astype(F32)

        def gathered(start, count):
            out = lax.dot_general(
                mixed[...], masks[start : start + count, :], (((1,), (1,)), ((), ())), preferred_element_type=F32
            )
            return (out[0:32] + out[32:64] + out[64:96]) * scale

        at_batch = gathered(0, batches)
        comp = lax.broadcasted_iota(jnp.int32, (32, batches), 0)
        degree = sum((comp >= (l + 1) * (l + 1)).astype(F32) for l in range(4))
        damped = jnp.where(comp < harmonics, at_batch * (mixing_beta / (1.0 + degree)), 0.0)
        lane_b = lax.broadcasted_iota(jnp.int32, (32, batches), 1)

        def density_step(step, carry):
            for u in range(4):
                b = step * 4 + u
                col = jnp.sum(jnp.where(lane_b == b, damped, 0.0), axis=1, keepdims=True)
                for v in range(per_batch):
                    t = b * per_batch + v
                    part = coeff_col * (rho[:, lane_tile(t)] + mixing_beta * res[:, lane_tile(t)])
                    for g in range(3):
                        part = part - col[g * SUBS : (g + 1) * SUBS] * basis[g * SUBS : (g + 1) * SUBS, lane_tile(t)]
                    part = part - col[24:32] * basis[24:25, lane_tile(t)]
                    density_out[pl.ds(t, 1), :] = jnp.sum(part, axis=0, keepdims=True)
            return carry

        lax.fori_loop(0, batches // 4, density_step, 0)
        if last:
            moments_out[...] = gathered(batches, owned)[0:harmonics]
        else:
            density = density_out[...]
            new = target[...] + coupling[...] * jnp.tanh(density) - density
            fresh[...] = new
            fresh_w[...] = new * w[...]


def local(weights, target, coupling, multipole_basis, rho_hist, res_hist, batch_atom, owner_slot, slot_index):
    harmonics, points = multipole_basis.shape
    hist_len = res_hist.shape[0]
    batches = batch_atom.shape[0]
    groups = lax.axis_size("grid")
    members = lax.axis_size("atom")
    devices = groups * members
    owned = owner_slot.shape[0] // members
    scale = 1.0 / math.sqrt(points * groups // owned)
    iters = slot_index.shape[0]
    cfg = (iters, hist_len, harmonics, batches, points // batches, owned, groups, members, scale)
    tiles = points // LANES
    flat = (tiles, LANES)
    any_space = pl.BlockSpec(memory_space=pl.ANY)
    smem = pl.BlockSpec(memory_space=pltpu.SMEM)
    vmem = pl.BlockSpec(memory_space=pltpu.VMEM)
    density, moments = pl.pallas_call(
        functools.partial(kernel, cfg),
        out_shape=(jax.ShapeDtypeStruct(flat, F32), jax.ShapeDtypeStruct((harmonics, owned), F32)),
        in_specs=[smem] * 3 + [any_space] * 6,
        out_specs=(vmem, vmem),
        scratch_shapes=[
            pltpu.VMEM(flat, F32),
            pltpu.VMEM(flat, F32),
            pltpu.VMEM(flat, F32),
            pltpu.VMEM((harmonics, points), F32),
            pltpu.VMEM((hist_len, points), F32),
            pltpu.VMEM((hist_len, points), F32),
            pltpu.VMEM(flat, F32),
            pltpu.VMEM(flat, F32),
            pltpu.VMEM((iters, devices, 1, LANES), F32),
            pltpu.VMEM((iters, devices, 2 * SUBS, LANES), F32),
            pltpu.VMEM((batches + owned, devices * batches), jnp.bfloat16),
            pltpu.VMEM((96, devices * batches), jnp.bfloat16),
            pltpu.SemaphoreType.DMA((6,)),
            pltpu.SemaphoreType.DMA((2 * iters, devices)),
            pltpu.SemaphoreType.DMA((2 * iters, devices)),
        ],
        compiler_params=pltpu.CompilerParams(
            collective_id=0, has_side_effects=True, vmem_limit_bytes=48 * 1024 * 1024
        ),
    )(
        batch_atom,
        owner_slot,
        slot_index,
        weights.reshape(flat),
        target.reshape(flat),
        coupling.reshape(flat),
        multipole_basis,
        rho_hist,
        res_hist,
    )
    return density.reshape(points), moments


def solution(mesh):
    both = ("grid", "atom")
    placed = (P(both), P(both), P(both), P(None, both), P(None, both), P(None, both), P(both), P(), P())
    return jax.shard_map(
        local,
        mesh=mesh,
        in_specs=placed,
        out_specs=(P(both), P(None, "atom")),
        check_vma=False,
    )
```

```python
import functools
import math

import jax
import jax.numpy as jnp
from jax import lax
from jax.experimental import pallas as pl
from jax.experimental.pallas import tpu as pltpu
from jax.sharding import PartitionSpec as P

MESH = pl.DeviceIdType.MESH
LANES = 128
SUBS = 8
mixing_beta = 0.5
ridge_share = 0.1
F32 = jnp.float32


def solve_coeffs(entry, hist_len):
    trace = entry[0][0]
    for i in range(1, hist_len):
        trace = trace + entry[i][i]
    ridge = (ridge_share / hist_len) * trace
    low = [[entry[i][j] for j in range(i + 1)] for i in range(hist_len)]
    for i in range(hist_len):
        low[i][i] = low[i][i] + ridge
    inverse = [None] * hist_len
    factor = [[None] * hist_len for _ in range(hist_len)]
    forward = [jnp.ones_like(trace) for _ in range(hist_len)]
    for j in range(hist_len):
        inverse[j] = 1.0 / low[j][j]
        for i in range(j + 1, hist_len):
            factor[i][j] = low[i][j] * inverse[j]
        for i in range(j + 1, hist_len):
            forward[i] = forward[i] - factor[i][j] * forward[j]
            for k in range(j + 1, i + 1):
                low[i][k] = low[i][k] - factor[i][j] * low[k][j]
    backward = [forward[i] * inverse[i] for i in range(hist_len)]
    for j in reversed(range(hist_len)):
        for i in range(j):
            backward[i] = backward[i] - factor[j][i] * backward[j]
    total = backward[0]
    for i in range(1, hist_len):
        total = total + backward[i]
    return [backward[i] / total for i in range(hist_len)]


def split(x):
    pieces = []
    for _ in range(3):
        piece = x.astype(jnp.bfloat16).astype(F32)
        pieces.append(piece)
        x = x - piece
    return pieces


def kernel(
    cfg,
    batch_atom,
    owner_slot,
    slot_index,
    w_hbm,
    target_hbm,
    coupling_hbm,
    basis_hbm,
    rho_hbm,
    res_hbm,
    density_out,
    moments_out,
    w,
    target,
    coupling,
    basis,
    rho,
    res,
    fresh,
    fresh_w,
    row_bufs,
    moment_bufs,
    near,
    own,
    hist_moments,
    base_rows,
    correct,
    load_sem,
    send_sem,
    recv_sem,
):
    iters, hist_len, harmonics, batches, width, owned, groups, members, scale = cfg
    devices = groups * members
    tiles = w.shape[0]
    per_batch = width // LANES
    half = LANES // 2
    rows = batches // 4
    my_group = lax.axis_index("grid")
    my_member = lax.axis_index("atom")
    me = my_group * members + my_member

    def peer(step):
        spot = lax.rem(me + step, devices)
        return spot, (lax.div(spot, members), lax.rem(spot, members))

    barrier = pltpu.get_barrier_semaphore()

    @pl.loop(1, devices)
    def _(step):
        pl.semaphore_signal(barrier, inc=1, device_id=peer(step)[1], device_id_type=MESH)

    loads = [
        pltpu.make_async_copy(src, dst, load_sem.at[k])
        for k, (src, dst) in enumerate(
            ((res_hbm, res), (w_hbm, w), (basis_hbm, basis), (rho_hbm, rho), (target_hbm, target), (coupling_hbm, coupling))
        )
    ]
    for load in loads:
        load.start()

    lane = lax.broadcasted_iota(jnp.int32, (SUBS, LANES), 1)
    sub = lax.broadcasted_iota(jnp.int32, (SUBS, LANES), 0)
    quarter = lane // 32
    lane_row = lax.broadcasted_iota(jnp.int32, (1, LANES), 1)

    slot_row = jnp.zeros((1, LANES), F32)
    slot_cols = []
    for block in range(batches // SUBS):
        col = jnp.zeros((SUBS, LANES), F32)
        for at in range(SUBS):
            b = block * SUBS + at
            slot = owner_slot[batch_atom[b]].astype(F32)
            slot_row = jnp.where(lane_row == half + b, slot, slot_row)
            col = jnp.where(sub == at, slot, col)
        slot_cols.append(col)
    slot_col = jnp.concatenate(slot_cols, axis=0)

    def lane_tile(t):
        return pl.ds(pl.multiple_of(t * LANES, LANES), LANES)

    def exchange(buf, which):
        def copy(step, spot):
            dst, device = peer(step)
            return pltpu.make_async_remote_copy(
                src_ref=buf.at[me],
                dst_ref=buf.at[spot],
                send_sem=send_sem.at[which, step],
                recv_sem=recv_sem.at[which, spot],
                device_id=device,
                device_id_type=MESH,
            )

        @pl.loop(1, devices)
        def _(step):
            copy(step, me).start()

        def wait():
            @pl.loop(1, devices)
            def _(step):
                copy(step, lax.rem(me - step + devices, devices)).wait_recv()

            @pl.loop(1, devices)
            def _(step):
                copy(step, me).wait_send()

        return wait

    def total_row(buf):
        total = buf[0]
        for spot in range(1, devices):
            total = total + buf[spot]
        return total

    def splat(row, k):
        return jnp.broadcast_to(row[:, k : k + 1], (1, LANES))

    shifts = hist_len // 2 + 1
    entry = None
    for iteration in range(iters):
        row_buf = row_bufs.at[iteration]
        moment_buf = moment_bufs.at[iteration]
        last = iteration == iters - 1

        if iteration == 0:
            loads[0].wait()
            loads[1].wait()

            def gram(step, acc):
                acc = list(acc)
                for u in range(8):
                    t = step * 8 + u
                    x = res[:, lane_tile(t)]
                    y = x * w[pl.ds(t, 1), :]
                    for r in range(shifts):
                        acc[r] = acc[r] + y * (pltpu.roll(x, r, 0) if r else x)
                return tuple(acc)

            acc = lax.fori_loop(0, tiles // 8, gram, tuple(jnp.zeros((SUBS, LANES), F32) for _ in range(shifts)))
            packed = jnp.zeros((SUBS, LANES), F32)
            for r in range(shifts):
                packed = jnp.where(lane == hist_len * r + sub, jnp.sum(acc[r], axis=1, keepdims=True), packed)
            row_buf[pl.ds(me, 1)] = (jnp.sum(packed, axis=0, keepdims=True) + slot_row)[None]
            pl.semaphore_wait(barrier, devices - 1)
        else:
            slot = slot_index[iteration - 1]
            replaced = sub == slot

            def refresh(step, acc):
                for u in range(8):
                    t = step * 8 + u
                    new_res = jnp.where(replaced, fresh[pl.ds(t, 1), :], res[:, lane_tile(t)])
                    new_rho = jnp.where(replaced, density_out[pl.ds(t, 1), :], rho[:, lane_tile(t)])
                    res[:, lane_tile(t)] = new_res
                    rho[:, lane_tile(t)] = new_rho
                    acc = acc + fresh_w[pl.ds(t, 1), :] * new_res
                return acc

            acc = lax.fori_loop(0, tiles // 8, refresh, jnp.zeros((SUBS, LANES), F32))
            packed = jnp.where(lane == sub, jnp.sum(acc, axis=1, keepdims=True), 0.0)
            row_buf[pl.ds(me, 1)] = jnp.sum(packed, axis=0, keepdims=True)[None]
        wait = exchange(row_buf, 2 * iteration)

        if iteration == 0:
            loads[2].wait()

        @pl.loop(0, rows)
        def _(r):
            xs, ys = [], []
            for q in range(4):
                b = q * rows + r
                at = pl.ds(pl.multiple_of(b * width, width), width)
                gain = jnp.concatenate([w[pl.ds(b * per_batch + v, 1), :] for v in range(per_batch)], axis=1)
                xs.extend(split(res[:, at] * gain))
                ys.append(jnp.concatenate([basis[0:24, at], jnp.broadcast_to(basis[24:25, at], (SUBS, width))], axis=0))
            x = jnp.concatenate(xs, axis=0).astype(jnp.bfloat16)
            out = None
            for y in split(jnp.concatenate(ys, axis=0)):
                part = lax.dot_general(
                    x, y.astype(jnp.bfloat16), (((1,), (1,)), ((), ())), preferred_element_type=F32
                )
                out = part if out is None else out + part
            tile = jnp.zeros((SUBS, LANES), F32)
            for q in range(4):
                block = out[24 * q : 24 * q + 8] + out[24 * q + 8 : 24 * q + 16] + out[24 * q + 16 : 24 * q + 24]
                tile = jnp.where(quarter == q, block, tile)
            hist_moments[r] = tile

        wait()

        row = total_row(row_buf)
        if iteration == 0:
            entry = [[None] * (i + 1) for i in range(hist_len)]
            for i in range(hist_len):
                for j in range(i + 1):
                    r = i - j
                    at = hist_len * r + i if r < shifts else hist_len * (hist_len - r) + j
                    entry[i][j] = splat(row, at)
        else:
            news = [splat(row, k) for k in range(hist_len)]
            slot_vec = jnp.zeros((1, LANES), jnp.int32) + slot
            entry = [
                [
                    jnp.where(slot_vec == i, news[j], jnp.where(slot_vec == j, news[i], entry[i][j]))
                    for j in range(i + 1)
                ]
                for i in range(hist_len)
            ]
        coeffs = solve_coeffs(entry, hist_len)
        coeff_col = jnp.zeros((SUBS, LANES), F32)
        for i in range(hist_len):
            coeff_col = jnp.where(sub == i, coeffs[i], coeff_col)

        mixed = [jnp.sum(coeff_col * hist_moments[r], axis=0, keepdims=True) for r in range(rows)]
        moment_buf[pl.ds(me, 1)] = jnp.concatenate(mixed, axis=0)[None]
        wait = exchange(moment_buf, 2 * iteration + 1)

        if iteration == 0:
            base = (my_member * owned).astype(F32)
            wide = lax.broadcasted_iota(jnp.int32, (owned, LANES), 0).astype(F32) + base

            @pl.loop(0, devices // SUBS)
            def _(c):
                ids = jnp.concatenate([row_buf[c * SUBS + i] for i in range(SUBS)], axis=0)
                stepped = pltpu.roll(ids, 0, 1, stride=rows, stride_axis=0)
                for q in range(4):
                    turned = pltpu.roll(stepped, (half - rows * q) % LANES, 1)
                    slots = jnp.sum(jnp.where(lane // rows == sub, turned, 0.0), axis=0, keepdims=True)
                    near[q * batches : (q + 1) * batches, lane_tile(c)] = jnp.where(
                        slot_col == slots, 1.0, 0.0
                    ).astype(jnp.bfloat16)
                    own[q * owned : (q + 1) * owned, lane_tile(c)] = jnp.where(wide == slots, 1.0, 0.0).astype(
                        jnp.bfloat16
                    )

            for load in loads[3:]:
                load.wait()

        def base_step(step, carry):
            for u in range(8):
                t = step * 8 + u
                part = coeff_col * (rho[:, lane_tile(t)] + mixing_beta * res[:, lane_tile(t)])
                base_rows[pl.ds(t, 1), :] = jnp.sum(part, axis=0, keepdims=True)
            return carry

        lax.fori_loop(0, tiles // 8, base_step, 0)
        wait()

        everywhere = moment_buf[...].reshape(devices * rows, LANES)
        pieces = jnp.concatenate([piece.astype(jnp.bfloat16) for piece in split(everywhere)], axis=1)

        def gathered(mask, count):
            out = jnp.dot(mask[...], pieces, preferred_element_type=F32)
            out = out[:, 0:LANES] + out[:, LANES : 2 * LANES] + out[:, 2 * LANES :]
            group = lax.broadcasted_iota(jnp.int32, (count, LANES), 1) // 32
            total = out[0:count]
            for q in range(1, 4):
                total = jnp.where(group == q, out[q * count : (q + 1) * count], total)
            total = total + pltpu.roll(total, 64, 1)
            total = total + pltpu.roll(total, 32, 1)
            return jnp.transpose(total)[0:32] * scale

        at_batch = gathered(near, batches)
        comp = lax.broadcasted_iota(jnp.int32, (32, batches), 0)
        degree = sum((comp >= (l + 1) * (l + 1)).astype(F32) for l in range(4))
        damped = jnp.where(comp < harmonics, at_batch * (mixing_beta / (1.0 + degree)), 0.0)
        lane_b = lax.broadcasted_iota(jnp.int32, (32, batches), 1)

        def density_step(step, carry):
            for u in range(4):
                b = step * 4 + u
                col = jnp.sum(jnp.where(lane_b == b, damped, 0.0), axis=1, keepdims=True)
                for v in range(per_batch):
                    t = b * per_batch + v
                    part = col[24:32] * basis[24:25, lane_tile(t)]
                    for g in range(3):
                        part = part + col[g * SUBS : (g + 1) * SUBS] * basis[g * SUBS : (g + 1) * SUBS, lane_tile(t)]
                    correct[pl.ds(t, 1), :] = jnp.sum(part, axis=0, keepdims=True)
            return carry

        lax.fori_loop(0, batches // 4, density_step, 0)
        density = base_rows[...] - correct[...]
        density_out[...] = density
        if last:
            moments_out[...] = gathered(own, owned)[0:harmonics]
        else:
            new = target[...] + coupling[...] * jnp.tanh(density) - density
            fresh[...] = new
            fresh_w[...] = new * w[...]


def local(weights, target, coupling, multipole_basis, rho_hist, res_hist, batch_atom, owner_slot, slot_index):
    harmonics, points = multipole_basis.shape
    hist_len = res_hist.shape[0]
    batches = batch_atom.shape[0]
    groups = lax.axis_size("grid")
    members = lax.axis_size("atom")
    devices = groups * members
    owned = owner_slot.shape[0] // members
    scale = 1.0 / math.sqrt(points * groups // owned)
    iters = slot_index.shape[0]
    cfg = (iters, hist_len, harmonics, batches, points // batches, owned, groups, members, scale)
    tiles = points // LANES
    flat = (tiles, LANES)
    any_space = pl.BlockSpec(memory_space=pl.ANY)
    smem = pl.BlockSpec(memory_space=pltpu.SMEM)
    vmem = pl.BlockSpec(memory_space=pltpu.VMEM)
    density, moments = pl.pallas_call(
        functools.partial(kernel, cfg),
        out_shape=(jax.ShapeDtypeStruct(flat, F32), jax.ShapeDtypeStruct((harmonics, owned), F32)),
        in_specs=[smem] * 3 + [any_space] * 6,
        out_specs=(vmem, vmem),
        scratch_shapes=[
            pltpu.VMEM(flat, F32),
            pltpu.VMEM(flat, F32),
            pltpu.VMEM(flat, F32),
            pltpu.VMEM((harmonics, points), F32),
            pltpu.VMEM((hist_len, points), F32),
            pltpu.VMEM((hist_len, points), F32),
            pltpu.VMEM(flat, F32),
            pltpu.VMEM(flat, F32),
            pltpu.VMEM((iters, devices, 1, LANES), F32),
            pltpu.VMEM((iters, devices, batches // 4, LANES), F32),
            pltpu.VMEM((4 * batches, devices * batches // 4), jnp.bfloat16),
            pltpu.VMEM((4 * owned, devices * batches // 4), jnp.bfloat16),
            pltpu.VMEM((batches // 4, SUBS, LANES), F32),
            pltpu.VMEM(flat, F32),
            pltpu.VMEM(flat, F32),
            pltpu.SemaphoreType.DMA((6,)),
            pltpu.SemaphoreType.DMA((2 * iters, devices)),
            pltpu.SemaphoreType.DMA((2 * iters, devices)),
        ],
        compiler_params=pltpu.CompilerParams(
            collective_id=0, has_side_effects=True, vmem_limit_bytes=67043328
        ),
    )(
        batch_atom,
        owner_slot,
        slot_index,
        weights.reshape(flat),
        target.reshape(flat),
        coupling.reshape(flat),
        multipole_basis,
        rho_hist,
        res_hist,
    )
    return density.reshape(points), moments


def solution(mesh):
    both = ("grid", "atom")
    placed = (P(both), P(both), P(both), P(None, both), P(None, both), P(None, both), P(both), P(), P())
    return jax.shard_map(
        local,
        mesh=mesh,
        in_specs=placed,
        out_specs=(P(both), P(None, "atom")),
        check_vma=False,
    )
```

```python
import functools
import math

import jax
import jax.numpy as jnp
from jax import lax
from jax.experimental import pallas as pl
from jax.experimental.pallas import tpu as pltpu
from jax.sharding import PartitionSpec as P

MESH = pl.DeviceIdType.MESH
LANES = 128
SUBS = 8
mixing_beta = 0.5
ridge_share = 0.1
F32 = jnp.float32


def solve_coeffs(entry, hist_len):
    trace = entry[0][0]
    for i in range(1, hist_len):
        trace = trace + entry[i][i]
    ridge = (ridge_share / hist_len) * trace
    low = [[entry[i][j] for j in range(i + 1)] for i in range(hist_len)]
    for i in range(hist_len):
        low[i][i] = low[i][i] + ridge
    inverse = [None] * hist_len
    factor = [[None] * hist_len for _ in range(hist_len)]
    forward = [jnp.ones_like(trace) for _ in range(hist_len)]
    for j in range(hist_len):
        inverse[j] = 1.0 / low[j][j]
        for i in range(j + 1, hist_len):
            factor[i][j] = low[i][j] * inverse[j]
        for i in range(j + 1, hist_len):
            forward[i] = forward[i] - factor[i][j] * forward[j]
            for k in range(j + 1, i + 1):
                low[i][k] = low[i][k] - factor[i][j] * low[k][j]
    backward = [forward[i] * inverse[i] for i in range(hist_len)]
    for j in reversed(range(hist_len)):
        for i in range(j):
            backward[i] = backward[i] - factor[j][i] * backward[j]
    total = backward[0]
    for i in range(1, hist_len):
        total = total + backward[i]
    return [backward[i] / total for i in range(hist_len)]


def split(x):
    pieces = []
    for _ in range(3):
        piece = x.astype(jnp.bfloat16).astype(F32)
        pieces.append(piece)
        x = x - piece
    return pieces


def kernel(
    cfg,
    batch_atom,
    owner_slot,
    slot_index,
    w_hbm,
    target_hbm,
    coupling_hbm,
    basis_hbm,
    rho_hbm,
    res_hbm,
    density_out,
    moments_out,
    w,
    target,
    coupling,
    basis,
    rho,
    res,
    fresh,
    fresh_w,
    row_bufs,
    moment_bufs,
    near,
    own,
    hist_moments,
    base_rows,
    correct,
    load_sem,
    send_sem,
    recv_sem,
):
    iters, hist_len, harmonics, batches, width, owned, groups, members, scale = cfg
    devices = groups * members
    tiles = w.shape[0]
    per_batch = width // LANES
    half = LANES // 2
    rows = batches // 4
    my_group = lax.axis_index("grid")
    my_member = lax.axis_index("atom")
    me = my_group * members + my_member

    def peer(step):
        spot = lax.rem(me + step, devices)
        return spot, (lax.div(spot, members), lax.rem(spot, members))

    barrier = pltpu.get_barrier_semaphore()

    @pl.loop(1, devices)
    def _(step):
        pl.semaphore_signal(barrier, inc=1, device_id=peer(step)[1], device_id_type=MESH)

    loads = [
        pltpu.make_async_copy(src, dst, load_sem.at[k])
        for k, (src, dst) in enumerate(
            ((res_hbm, res), (w_hbm, w), (basis_hbm, basis), (rho_hbm, rho), (target_hbm, target), (coupling_hbm, coupling))
        )
    ]
    for load in loads:
        load.start()

    lane = lax.broadcasted_iota(jnp.int32, (SUBS, LANES), 1)
    sub = lax.broadcasted_iota(jnp.int32, (SUBS, LANES), 0)
    quarter = lane // 32
    lane_row = lax.broadcasted_iota(jnp.int32, (1, LANES), 1)

    slot_row = jnp.zeros((1, LANES), F32)
    slot_cols = []
    for block in range(batches // SUBS):
        col = jnp.zeros((SUBS, LANES), F32)
        for at in range(SUBS):
            b = block * SUBS + at
            slot = owner_slot[batch_atom[b]].astype(F32)
            slot_row = jnp.where(lane_row == half + b, slot, slot_row)
            col = jnp.where(sub == at, slot, col)
        slot_cols.append(col)
    slot_col = jnp.concatenate(slot_cols, axis=0)

    def lane_tile(t):
        return pl.ds(pl.multiple_of(t * LANES, LANES), LANES)

    def exchange(buf, which):
        def copy(step, spot):
            dst, device = peer(step)
            return pltpu.make_async_remote_copy(
                src_ref=buf.at[me],
                dst_ref=buf.at[spot],
                send_sem=send_sem.at[which, step],
                recv_sem=recv_sem.at[which, spot],
                device_id=device,
                device_id_type=MESH,
            )

        @pl.loop(1, devices)
        def _(step):
            copy(step, me).start()

        def wait():
            @pl.loop(1, devices)
            def _(step):
                copy(step, lax.rem(me - step + devices, devices)).wait_recv()

            @pl.loop(1, devices)
            def _(step):
                copy(step, me).wait_send()

        return wait

    def total_row(buf):
        total = buf[0]
        for spot in range(1, devices):
            total = total + buf[spot]
        return total

    def splat(row, k):
        return jnp.broadcast_to(row[:, k : k + 1], (1, LANES))

    shifts = hist_len // 2 + 1
    entry = None
    for iteration in range(iters):
        row_buf = row_bufs.at[iteration]
        moment_buf = moment_bufs.at[iteration]
        last = iteration == iters - 1

        if iteration == 0:
            loads[0].wait()
            loads[1].wait()

            def gram(step, acc):
                acc = list(acc)
                for u in range(8):
                    t = step * 8 + u
                    x = res[:, lane_tile(t)]
                    y = x * w[pl.ds(t, 1), :]
                    for r in range(shifts):
                        acc[r] = acc[r] + y * (pltpu.roll(x, r, 0) if r else x)
                return tuple(acc)

            acc = lax.fori_loop(0, tiles // 8, gram, tuple(jnp.zeros((SUBS, LANES), F32) for _ in range(shifts)))
            packed = jnp.zeros((SUBS, LANES), F32)
            for r in range(shifts):
                packed = jnp.where(lane == hist_len * r + sub, jnp.sum(acc[r], axis=1, keepdims=True), packed)
            row_buf[pl.ds(me, 1)] = (jnp.sum(packed, axis=0, keepdims=True) + slot_row)[None]
            pl.semaphore_wait(barrier, devices - 1)
        else:
            slot = slot_index[iteration - 1]
            replaced = sub == slot

            def refresh(step, acc):
                for u in range(8):
                    t = step * 8 + u
                    new_res = jnp.where(replaced, fresh[pl.ds(t, 1), :], res[:, lane_tile(t)])
                    new_rho = jnp.where(replaced, density_out[pl.ds(t, 1), :], rho[:, lane_tile(t)])
                    res[:, lane_tile(t)] = new_res
                    rho[:, lane_tile(t)] = new_rho
                    acc = acc + fresh_w[pl.ds(t, 1), :] * new_res
                return acc

            acc = lax.fori_loop(0, tiles // 8, refresh, jnp.zeros((SUBS, LANES), F32))
            packed = jnp.where(lane == sub, jnp.sum(acc, axis=1, keepdims=True), 0.0)
            row_buf[pl.ds(me, 1)] = jnp.sum(packed, axis=0, keepdims=True)[None]
        wait = exchange(row_buf, 2 * iteration)

        if iteration == 0:
            loads[2].wait()

        @pl.loop(0, rows)
        def _(r):
            xs, ys = [], []
            for q in range(4):
                b = q * rows + r
                at = pl.ds(pl.multiple_of(b * width, width), width)
                gain = jnp.concatenate([w[pl.ds(b * per_batch + v, 1), :] for v in range(per_batch)], axis=1)
                xs.extend(split(res[:, at] * gain))
                ys.append(jnp.concatenate([basis[0:24, at], jnp.broadcast_to(basis[24:25, at], (SUBS, width))], axis=0))
            x = jnp.concatenate(xs, axis=0).astype(jnp.bfloat16)
            out = None
            for y in split(jnp.concatenate(ys, axis=0)):
                part = lax.dot_general(
                    x, y.astype(jnp.bfloat16), (((1,), (1,)), ((), ())), preferred_element_type=F32
                )
                out = part if out is None else out + part
            tile = jnp.zeros((SUBS, LANES), F32)
            for q in range(4):
                block = out[24 * q : 24 * q + 8] + out[24 * q + 8 : 24 * q + 16] + out[24 * q + 16 : 24 * q + 24]
                tile = jnp.where(quarter == q, block, tile)
            hist_moments[r] = tile

        wait()

        row = total_row(row_buf)
        if iteration == 0:
            entry = [[None] * (i + 1) for i in range(hist_len)]
            for i in range(hist_len):
                for j in range(i + 1):
                    r = i - j
                    at = hist_len * r + i if r < shifts else hist_len * (hist_len - r) + j
                    entry[i][j] = splat(row, at)
        else:
            news = [splat(row, k) for k in range(hist_len)]
            slot_vec = jnp.zeros((1, LANES), jnp.int32) + slot
            entry = [
                [
                    jnp.where(slot_vec == i, news[j], jnp.where(slot_vec == j, news[i], entry[i][j]))
                    for j in range(i + 1)
                ]
                for i in range(hist_len)
            ]
        coeffs = solve_coeffs(entry, hist_len)
        coeff_col = jnp.zeros((SUBS, LANES), F32)
        for i in range(hist_len):
            coeff_col = jnp.where(sub == i, coeffs[i], coeff_col)

        mixed = [jnp.sum(coeff_col * hist_moments[r], axis=0, keepdims=True) for r in range(rows)]
        moment_buf[pl.ds(me, 1)] = jnp.concatenate(mixed, axis=0)[None]
        wait = exchange(moment_buf, 2 * iteration + 1)

        if iteration == 0:
            base = (my_member * owned).astype(F32)
            wide = lax.broadcasted_iota(jnp.int32, (owned, LANES), 0).astype(F32) + base

            @pl.loop(0, devices // SUBS)
            def _(c):
                ids = jnp.concatenate([row_buf[c * SUBS + i] for i in range(SUBS)], axis=0)
                stepped = pltpu.roll(ids, 0, 1, stride=rows, stride_axis=0)
                for q in range(4):
                    turned = pltpu.roll(stepped, (half - rows * q) % LANES, 1)
                    slots = jnp.sum(jnp.where(lane // rows == sub, turned, 0.0), axis=0, keepdims=True)
                    near[q * batches : (q + 1) * batches, lane_tile(c)] = jnp.where(
                        slot_col == slots, 1.0, 0.0
                    ).astype(jnp.bfloat16)
                    own[q * owned : (q + 1) * owned, lane_tile(c)] = jnp.where(wide == slots, 1.0, 0.0).astype(
                        jnp.bfloat16
                    )

            for load in loads[3:]:
                load.wait()

        def base_step(step, carry):
            for u in range(8):
                t = step * 8 + u
                part = coeff_col * (rho[:, lane_tile(t)] + mixing_beta * res[:, lane_tile(t)])
                base_rows[pl.ds(t, 1), :] = jnp.sum(part, axis=0, keepdims=True)
            return carry

        lax.fori_loop(0, tiles // 8, base_step, 0)
        wait()

        everywhere = moment_buf[...].reshape(devices * rows, LANES)
        pieces = jnp.concatenate([piece.astype(jnp.bfloat16) for piece in split(everywhere)], axis=1)

        def gathered(mask, count):
            out = jnp.dot(mask[...], pieces, preferred_element_type=F32)
            out = out[:, 0:LANES] + out[:, LANES : 2 * LANES] + out[:, 2 * LANES :]
            group = lax.broadcasted_iota(jnp.int32, (count, LANES), 1) // 32
            total = out[0:count]
            for q in range(1, 4):
                total = jnp.where(group == q, out[q * count : (q + 1) * count], total)
            total = total + pltpu.roll(total, 64, 1)
            total = total + pltpu.roll(total, 32, 1)
            return jnp.transpose(jnp.concatenate([total] * max(1, LANES // count), axis=0))[0:32] * scale

        at_batch = gathered(near, batches)
        comp = lax.broadcasted_iota(jnp.int32, (32, LANES), 0)
        degree = sum((comp >= (l + 1) * (l + 1)).astype(F32) for l in range(4))
        damped = jnp.where(comp < harmonics, at_batch * (mixing_beta / (1.0 + degree)), 0.0)

        def density_step(step, ahead):
            for u in range(8):
                b = step * 8 + u
                col = jnp.broadcast_to(ahead[:, u : u + 1], (32, LANES))
                for v in range(per_batch):
                    t = b * per_batch + v
                    part = col[24:32] * basis[24:25, lane_tile(t)]
                    for g in range(3):
                        part = part + col[g * SUBS : (g + 1) * SUBS] * basis[g * SUBS : (g + 1) * SUBS, lane_tile(t)]
                    correct[pl.ds(t, 1), :] = jnp.sum(part, axis=0, keepdims=True)
            return pltpu.roll(ahead, LANES - 8, 1)

        lax.fori_loop(0, batches // 8, density_step, damped)
        density = base_rows[...] - correct[...]
        density_out[...] = density
        if last:
            moments_out[...] = gathered(own, owned)[0:harmonics]
        else:
            new = target[...] + coupling[...] * jnp.tanh(density) - density
            fresh[...] = new
            fresh_w[...] = new * w[...]


def local(weights, target, coupling, multipole_basis, rho_hist, res_hist, batch_atom, owner_slot, slot_index):
    harmonics, points = multipole_basis.shape
    hist_len = res_hist.shape[0]
    batches = batch_atom.shape[0]
    groups = lax.axis_size("grid")
    members = lax.axis_size("atom")
    devices = groups * members
    owned = owner_slot.shape[0] // members
    scale = 1.0 / math.sqrt(points * groups // owned)
    iters = slot_index.shape[0]
    cfg = (iters, hist_len, harmonics, batches, points // batches, owned, groups, members, scale)
    tiles = points // LANES
    flat = (tiles, LANES)
    any_space = pl.BlockSpec(memory_space=pl.ANY)
    smem = pl.BlockSpec(memory_space=pltpu.SMEM)
    vmem = pl.BlockSpec(memory_space=pltpu.VMEM)
    density, moments = pl.pallas_call(
        functools.partial(kernel, cfg),
        out_shape=(jax.ShapeDtypeStruct(flat, F32), jax.ShapeDtypeStruct((harmonics, owned), F32)),
        in_specs=[smem] * 3 + [any_space] * 6,
        out_specs=(vmem, vmem),
        scratch_shapes=[
            pltpu.VMEM(flat, F32),
            pltpu.VMEM(flat, F32),
            pltpu.VMEM(flat, F32),
            pltpu.VMEM((harmonics, points), F32),
            pltpu.VMEM((hist_len, points), F32),
            pltpu.VMEM((hist_len, points), F32),
            pltpu.VMEM(flat, F32),
            pltpu.VMEM(flat, F32),
            pltpu.VMEM((iters, devices, 1, LANES), F32),
            pltpu.VMEM((iters, devices, batches // 4, LANES), F32),
            pltpu.VMEM((4 * batches, devices * batches // 4), jnp.bfloat16),
            pltpu.VMEM((4 * owned, devices * batches // 4), jnp.bfloat16),
            pltpu.VMEM((batches // 4, SUBS, LANES), F32),
            pltpu.VMEM(flat, F32),
            pltpu.VMEM(flat, F32),
            pltpu.SemaphoreType.DMA((6,)),
            pltpu.SemaphoreType.DMA((2 * iters, devices)),
            pltpu.SemaphoreType.DMA((2 * iters, devices)),
        ],
        compiler_params=pltpu.CompilerParams(
            collective_id=0, has_side_effects=True, vmem_limit_bytes=67043328
        ),
    )(
        batch_atom,
        owner_slot,
        slot_index,
        weights.reshape(flat),
        target.reshape(flat),
        coupling.reshape(flat),
        multipole_basis,
        rho_hist,
        res_hist,
    )
    return density.reshape(points), moments


def solution(mesh):
    both = ("grid", "atom")
    placed = (P(both), P(both), P(both), P(None, both), P(None, both), P(None, both), P(both), P(), P())
    return jax.shard_map(
        local,
        mesh=mesh,
        in_specs=placed,
        out_specs=(P(both), P(None, "atom")),
        check_vma=False,
    )
```

```python
import functools
import math

import jax
import jax.numpy as jnp
from jax import lax
from jax.experimental import pallas as pl
from jax.experimental.pallas import tpu as pltpu
from jax.sharding import PartitionSpec as P

MESH = pl.DeviceIdType.MESH
LANES = 128
SUBS = 8
mixing_beta = 0.5
ridge_share = 0.1
F32 = jnp.float32


def solve_coeffs(entry, hist_len):
    trace = entry[0][0]
    for i in range(1, hist_len):
        trace = trace + entry[i][i]
    ridge = (ridge_share / hist_len) * trace
    low = [[entry[i][j] for j in range(i + 1)] for i in range(hist_len)]
    for i in range(hist_len):
        low[i][i] = low[i][i] + ridge
    inverse = [None] * hist_len
    factor = [[None] * hist_len for _ in range(hist_len)]
    forward = [jnp.ones_like(trace) for _ in range(hist_len)]
    for j in range(hist_len):
        inverse[j] = 1.0 / low[j][j]
        for i in range(j + 1, hist_len):
            factor[i][j] = low[i][j] * inverse[j]
        for i in range(j + 1, hist_len):
            forward[i] = forward[i] - factor[i][j] * forward[j]
            for k in range(j + 1, i + 1):
                low[i][k] = low[i][k] - factor[i][j] * low[k][j]
    backward = [forward[i] * inverse[i] for i in range(hist_len)]
    for j in reversed(range(hist_len)):
        for i in range(j):
            backward[i] = backward[i] - factor[j][i] * backward[j]
    total = backward[0]
    for i in range(1, hist_len):
        total = total + backward[i]
    return [backward[i] / total for i in range(hist_len)]


def split(x):
    pieces = []
    for _ in range(3):
        piece = x.astype(jnp.bfloat16).astype(F32)
        pieces.append(piece)
        x = x - piece
    return pieces


def kernel(
    cfg,
    batch_atom,
    owner_slot,
    slot_index,
    w_hbm,
    target_hbm,
    coupling_hbm,
    basis_hbm,
    rho_hbm,
    res_hbm,
    density_out,
    moments_out,
    w,
    target,
    coupling,
    basis,
    rho,
    res,
    fresh,
    fresh_w,
    row_bufs,
    moment_bufs,
    near,
    own,
    hist_moments,
    base_rows,
    correct,
    load_sem,
    send_sem,
    recv_sem,
):
    iters, hist_len, harmonics, batches, width, owned, groups, members, scale = cfg
    devices = groups * members
    tiles = w.shape[0]
    per_batch = width // LANES
    half = LANES // 2
    rows = batches // 4
    my_group = lax.axis_index("grid")
    my_member = lax.axis_index("atom")
    me = my_group * members + my_member

    def peer(step):
        spot = lax.rem(me + step, devices)
        return spot, (lax.div(spot, members), lax.rem(spot, members))

    barrier = pltpu.get_barrier_semaphore()

    @pl.loop(1, devices)
    def _(step):
        pl.semaphore_signal(barrier, inc=1, device_id=peer(step)[1], device_id_type=MESH)

    loads = [
        pltpu.make_async_copy(src, dst, load_sem.at[k])
        for k, (src, dst) in enumerate(
            ((res_hbm, res), (w_hbm, w), (basis_hbm, basis), (rho_hbm, rho), (target_hbm, target), (coupling_hbm, coupling))
        )
    ]
    for load in loads:
        load.start()

    lane = lax.broadcasted_iota(jnp.int32, (SUBS, LANES), 1)
    sub = lax.broadcasted_iota(jnp.int32, (SUBS, LANES), 0)
    quarter = lane // 32
    lane_row = lax.broadcasted_iota(jnp.int32, (1, LANES), 1)

    slot_row = jnp.zeros((1, LANES), F32)
    slot_cols = []
    for block in range(batches // SUBS):
        col = jnp.zeros((SUBS, LANES), F32)
        for at in range(SUBS):
            b = block * SUBS + at
            slot = owner_slot[batch_atom[b]].astype(F32)
            slot_row = jnp.where(lane_row == half + b, slot, slot_row)
            col = jnp.where(sub == at, slot, col)
        slot_cols.append(col)
    slot_col = jnp.concatenate(slot_cols, axis=0)

    def lane_tile(t):
        return pl.ds(pl.multiple_of(t * LANES, LANES), LANES)

    def exchange(buf, which):
        def copy(step, spot):
            dst, device = peer(step)
            return pltpu.make_async_remote_copy(
                src_ref=buf.at[me],
                dst_ref=buf.at[spot],
                send_sem=send_sem.at[which, step],
                recv_sem=recv_sem.at[which, spot],
                device_id=device,
                device_id_type=MESH,
            )

        @pl.loop(1, devices)
        def _(step):
            copy(step, me).start()

        def wait():
            @pl.loop(1, devices)
            def _(step):
                copy(step, lax.rem(me - step + devices, devices)).wait_recv()

            @pl.loop(1, devices)
            def _(step):
                copy(step, me).wait_send()

        return wait

    def total_row(buf):
        total = buf[0]
        for spot in range(1, devices):
            total = total + buf[spot]
        return total

    def splat(row, k):
        return jnp.broadcast_to(row[:, k : k + 1], (1, LANES))

    shifts = hist_len // 2 + 1
    entry = None
    for iteration in range(iters):
        row_buf = row_bufs.at[iteration]
        moment_buf = moment_bufs.at[iteration]
        last = iteration == iters - 1

        if iteration == 0:
            loads[0].wait()
            loads[1].wait()

            def gram(step, acc):
                acc = list(acc)
                for u in range(8):
                    t = step * 8 + u
                    x = res[:, lane_tile(t)]
                    y = x * w[pl.ds(t, 1), :]
                    for r in range(shifts):
                        acc[r] = acc[r] + y * (pltpu.roll(x, r, 0) if r else x)
                return tuple(acc)

            acc = lax.fori_loop(0, tiles // 8, gram, tuple(jnp.zeros((SUBS, LANES), F32) for _ in range(shifts)))
            packed = jnp.zeros((SUBS, LANES), F32)
            for r in range(shifts):
                packed = jnp.where(lane == hist_len * r + sub, jnp.sum(acc[r], axis=1, keepdims=True), packed)
            row_buf[pl.ds(me, 1)] = (jnp.sum(packed, axis=0, keepdims=True) + slot_row)[None]
            pl.semaphore_wait(barrier, devices - 1)
        else:
            slot = slot_index[iteration - 1]
            replaced = sub == slot

            def refresh(step, acc):
                for u in range(8):
                    t = step * 8 + u
                    new_res = jnp.where(replaced, fresh[pl.ds(t, 1), :], res[:, lane_tile(t)])
                    new_rho = jnp.where(replaced, density_out[pl.ds(t, 1), :], rho[:, lane_tile(t)])
                    res[:, lane_tile(t)] = new_res
                    rho[:, lane_tile(t)] = new_rho
                    acc = acc + fresh_w[pl.ds(t, 1), :] * new_res
                return acc

            acc = lax.fori_loop(0, tiles // 8, refresh, jnp.zeros((SUBS, LANES), F32))
            packed = jnp.where(lane == sub, jnp.sum(acc, axis=1, keepdims=True), 0.0)
            row_buf[pl.ds(me, 1)] = jnp.sum(packed, axis=0, keepdims=True)[None]
        wait = exchange(row_buf, 2 * iteration)

        if iteration == 0:
            loads[2].wait()

        @pl.loop(0, rows)
        def _(r):
            xs, ys = [], []
            for q in range(4):
                b = q * rows + r
                at = pl.ds(pl.multiple_of(b * width, width), width)
                gain = jnp.concatenate([w[pl.ds(b * per_batch + v, 1), :] for v in range(per_batch)], axis=1)
                xs.extend(split(res[:, at] * gain))
                ys.append(jnp.concatenate([basis[0:24, at], jnp.broadcast_to(basis[24:25, at], (SUBS, width))], axis=0))
            x = jnp.concatenate(xs, axis=0).astype(jnp.bfloat16)
            out = None
            for y in split(jnp.concatenate(ys, axis=0)):
                part = lax.dot_general(
                    x, y.astype(jnp.bfloat16), (((1,), (1,)), ((), ())), preferred_element_type=F32
                )
                out = part if out is None else out + part
            tile = jnp.zeros((SUBS, LANES), F32)
            for q in range(4):
                block = out[24 * q : 24 * q + 8] + out[24 * q + 8 : 24 * q + 16] + out[24 * q + 16 : 24 * q + 24]
                tile = jnp.where(quarter == q, block, tile)
            hist_moments[r] = tile

        wait()

        row = total_row(row_buf)
        if iteration == 0:
            entry = [[None] * (i + 1) for i in range(hist_len)]
            for i in range(hist_len):
                for j in range(i + 1):
                    r = i - j
                    at = hist_len * r + i if r < shifts else hist_len * (hist_len - r) + j
                    entry[i][j] = splat(row, at)
        else:
            news = [splat(row, k) for k in range(hist_len)]
            slot_vec = jnp.zeros((1, LANES), jnp.int32) + slot
            entry = [
                [
                    jnp.where(slot_vec == i, news[j], jnp.where(slot_vec == j, news[i], entry[i][j]))
                    for j in range(i + 1)
                ]
                for i in range(hist_len)
            ]
        coeffs = solve_coeffs(entry, hist_len)
        coeff_col = jnp.zeros((SUBS, LANES), F32)
        for i in range(hist_len):
            coeff_col = jnp.where(sub == i, coeffs[i], coeff_col)

        mixed = [jnp.sum(coeff_col * hist_moments[r], axis=0, keepdims=True) for r in range(rows)]
        moment_buf[pl.ds(me, 1)] = jnp.concatenate(mixed, axis=0)[None]
        wait = exchange(moment_buf, 2 * iteration + 1)

        if iteration == 0:
            base = (my_member * owned).astype(F32)
            wide = lax.broadcasted_iota(jnp.int32, (owned, LANES), 0).astype(F32) + base

            @pl.loop(0, devices // SUBS)
            def _(c):
                ids = jnp.concatenate([row_buf[c * SUBS + i] for i in range(SUBS)], axis=0)
                stepped = pltpu.roll(ids, 0, 1, stride=rows, stride_axis=0)
                for q in range(4):
                    turned = pltpu.roll(stepped, (half - rows * q) % LANES, 1)
                    slots = jnp.sum(jnp.where(lane // rows == sub, turned, 0.0), axis=0, keepdims=True)
                    near[q * batches : (q + 1) * batches, lane_tile(c)] = jnp.where(
                        slot_col == slots, 1.0, 0.0
                    ).astype(jnp.bfloat16)
                    own[q * owned : (q + 1) * owned, lane_tile(c)] = jnp.where(wide == slots, 1.0, 0.0).astype(
                        jnp.bfloat16
                    )

            for load in loads[3:]:
                load.wait()

        def base_step(step, carry):
            for u in range(8):
                t = step * 8 + u
                part = coeff_col * (rho[:, lane_tile(t)] + mixing_beta * res[:, lane_tile(t)])
                base_rows[pl.ds(t, 1), :] = jnp.sum(part, axis=0, keepdims=True)
            return carry

        lax.fori_loop(0, tiles // 8, base_step, 0)
        wait()

        everywhere = moment_buf[...].reshape(devices * rows, LANES)
        pieces = jnp.concatenate([piece.astype(jnp.bfloat16) for piece in split(everywhere)], axis=1)

        def gathered(mask, count):
            out = jnp.dot(mask[...], pieces, preferred_element_type=F32)
            out = out[:, 0:LANES] + out[:, LANES : 2 * LANES] + out[:, 2 * LANES :]
            group = lax.broadcasted_iota(jnp.int32, (count, LANES), 1) // 32
            total = out[0:count]
            for q in range(1, 4):
                total = jnp.where(group == q, out[q * count : (q + 1) * count], total)
            total = total + pltpu.roll(total, 64, 1)
            total = total + pltpu.roll(total, 32, 1)
            return jnp.transpose(jnp.concatenate([total] * max(1, LANES // count), axis=0))[0:32] * scale

        at_batch = gathered(near, batches)
        comp = lax.broadcasted_iota(jnp.int32, (32, LANES), 0)
        degree = sum((comp >= (l + 1) * (l + 1)).astype(F32) for l in range(4))
        damped = jnp.where(comp < harmonics, at_batch * (mixing_beta / (1.0 + degree)), 0.0)

        def density_step(step, ahead):
            for u in range(16):
                b = step * 16 + u
                col = jnp.broadcast_to(ahead[:, u : u + 1], (32, LANES))
                for v in range(per_batch):
                    t = b * per_batch + v
                    part = col[24:32] * basis[24:25, lane_tile(t)]
                    for g in range(3):
                        part = part + col[g * SUBS : (g + 1) * SUBS] * basis[g * SUBS : (g + 1) * SUBS, lane_tile(t)]
                    correct[pl.ds(t, 1), :] = jnp.sum(part, axis=0, keepdims=True)
            return pltpu.roll(ahead, LANES - 16, 1)

        lax.fori_loop(0, batches // 16, density_step, damped)
        density = base_rows[...] - correct[...]
        density_out[...] = density
        if last:
            moments_out[...] = gathered(own, owned)[0:harmonics]
        else:
            new = target[...] + coupling[...] * jnp.tanh(density) - density
            fresh[...] = new
            fresh_w[...] = new * w[...]


def finish(density, moments, density_out, moments_out):
    density_out[...] = density[...]
    moments_out[...] = moments[...]


def local(weights, target, coupling, multipole_basis, rho_hist, res_hist, batch_atom, owner_slot, slot_index):
    harmonics, points = multipole_basis.shape
    hist_len = res_hist.shape[0]
    batches = batch_atom.shape[0]
    groups = lax.axis_size("grid")
    members = lax.axis_size("atom")
    devices = groups * members
    owned = owner_slot.shape[0] // members
    scale = 1.0 / math.sqrt(points * groups // owned)
    iters = slot_index.shape[0]
    cfg = (iters, hist_len, harmonics, batches, points // batches, owned, groups, members, scale)
    tiles = points // LANES
    flat = (tiles, LANES)
    any_space = pl.BlockSpec(memory_space=pl.ANY)
    smem = pl.BlockSpec(memory_space=pltpu.SMEM)
    vmem = pl.BlockSpec(memory_space=pltpu.VMEM)
    density, moments = pl.pallas_call(
        functools.partial(kernel, cfg),
        out_shape=(jax.ShapeDtypeStruct(flat, F32), jax.ShapeDtypeStruct((harmonics, owned), F32)),
        in_specs=[smem] * 3 + [any_space] * 6,
        out_specs=(vmem, vmem),
        scratch_shapes=[
            pltpu.VMEM(flat, F32),
            pltpu.VMEM(flat, F32),
            pltpu.VMEM(flat, F32),
            pltpu.VMEM((harmonics, points), F32),
            pltpu.VMEM((hist_len, points), F32),
            pltpu.VMEM((hist_len, points), F32),
            pltpu.VMEM(flat, F32),
            pltpu.VMEM(flat, F32),
            pltpu.VMEM((iters, devices, 1, LANES), F32),
            pltpu.VMEM((iters, devices, batches // 4, LANES), F32),
            pltpu.VMEM((4 * batches, devices * batches // 4), jnp.bfloat16),
            pltpu.VMEM((4 * owned, devices * batches // 4), jnp.bfloat16),
            pltpu.VMEM((batches // 4, SUBS, LANES), F32),
            pltpu.VMEM(flat, F32),
            pltpu.VMEM(flat, F32),
            pltpu.SemaphoreType.DMA((6,)),
            pltpu.SemaphoreType.DMA((2 * iters, devices)),
            pltpu.SemaphoreType.DMA((2 * iters, devices)),
        ],
        compiler_params=pltpu.CompilerParams(
            collective_id=0, has_side_effects=True, vmem_limit_bytes=67043328
        ),
    )(
        batch_atom,
        owner_slot,
        slot_index,
        weights.reshape(flat),
        target.reshape(flat),
        coupling.reshape(flat),
        multipole_basis,
        rho_hist,
        res_hist,
    )
    density, moments = pl.pallas_call(
        finish,
        out_shape=(jax.ShapeDtypeStruct(flat, F32), jax.ShapeDtypeStruct((harmonics, owned), F32)),
        in_specs=[vmem] * 2,
        out_specs=(vmem, vmem),
    )(density, moments)
    return density.reshape(points), moments


def solution(mesh):
    both = ("grid", "atom")
    placed = (P(both), P(both), P(both), P(None, both), P(None, both), P(None, both), P(both), P(), P())
    return jax.shard_map(
        local,
        mesh=mesh,
        in_specs=placed,
        out_specs=(P(both), P(None, "atom")),
        check_vma=False,
    )
```
